32 devices in a mesh: row: 4 (over x, core), col: 8 (over z, y).
Axes of the slice: x: 2, y: 2, z: 4, core: 2. Of those that a mesh axis runs over, the one named last changes fastest.
Arguments:
- velocity_start: float32 [2, 256, 1024], P(None, 'row', 'col'), may hold values from -3 to 3
- stress_start: float32 [3, 256, 1024], P(None, 'row', 'col'), may hold values from -3 to 3
- wind_stress: float32 [2, 256, 1024], P(None, 'row', 'col'), may hold values from -6 to 6
- ocean_current: float32 [2, 256, 1024], P(None, 'row', 'col'), may hold values from -3 to 3
- ice_area: float32 [5, 256, 1024], P(None, 'row', 'col'), may hold values from 0.15 to 0.2
- ice_volume: float32 [5, 256, 1024], P(None, 'row', 'col'), may hold values from 0.05 to 0.6
- inverse_width: float32 [256, 1024], P('row', 'col'), may hold values from 0.7 to 1.4
- inverse_height: float32 [256, 1024], P('row', 'col'), may hold values from 0.7 to 1.4
- land_block: int32 [64, 32], P('row', 'col'), may hold values 0 or 1
- ice_block: int32 [64, 32], P('row', 'col'), may hold values 0 or 1
- writer: int32 [8], replicated, may hold values from 0 to 3
Outputs:
- velocity: float32 [2, 256, 1024], P(None, 'row', 'col')
- stress: float32 [3, 256, 1024], P(None, 'row', 'col')
- restart: float32 [4, 10, 256, 1024], P('row', None, None, 'col')
The draws below stay inside these ranges and needn't reach their ends.
All inputs are finite; a program needn't handle non-finite values. No bound on the sum of `land_block` or of `ice_block` on one device may be relied on, other than what follows from the above.
Results may differ from the reference program's by a relative error of at most 0.00002.
Values sent between devices are 32-bit elements; how exact they have to be, the bound alone decides.
A program may use at most 64 MiB of HBM per device.

```python
import math
import jax
import jax.numpy as jnp
from jax import lax

CX = 128
NCAT = 5
SUB = 12
NY = 256
NX = 1024
NBY = 64
NBX = 32
GROUPS = 8
SLOTS = 4


def place_ends(array, key, least, high):
    spot = [jax.random.randint(jax.random.fold_in(key, axis), (), 0, length) for axis, length in enumerate(array.shape)]
    longest = array.shape.index(max(array.shape))
    neighbour = spot[:longest] + [(spot[longest] + 1) % array.shape[longest]] + spot[longest + 1:]
    return array.at[tuple(spot)].set(least).at[tuple(neighbour)].set(high)


def block_scale(rng, extent, pieces, least, largest):
    gain, own = 1.0, jax.random.fold_in(rng, 6)
    for axis_at, shards_of in pieces:
        draws = jnp.exp(jax.random.uniform(jax.random.fold_in(own, axis_at), (shards_of,), jnp.float32, least / len(pieces), largest / len(pieces)))
        gain = gain * jnp.repeat(draws, extent[axis_at] // shards_of).reshape([-1 if axis == axis_at else 1 for axis in range(len(extent))])
    return gain


def centred(stream_key, shape, scale, reach, cuts=(), held_as=jnp.bfloat16):
    array = jax.random.normal(stream_key, shape, jnp.float32) * scale
    if len(cuts) > 0:
        array = block_scale(stream_key, shape, cuts, -0.22, 0.18) * array
    return jnp.clip(array, min=-reach, max=reach).astype(held_as)


def setup_inputs(seed: int = 0) -> dict:
    splits = jax.random.split(jax.random.key(seed), 12)
    velocity_start = centred(splits[0], (2, NY, NX), 0.5, 3.0, ((1, 4), (2, 8)), jnp.float32)
    stress_start = centred(splits[1], (3, NY, NX), 0.5, 3.0, ((1, 4), (2, 8)), jnp.float32)
    wind_stress = centred(splits[2], (2, NY, NX), 1.0, 6.0, ((1, 4), (2, 8)), jnp.float32)
    ocean_current = centred(splits[3], (2, NY, NX), 0.5, 3.0, ((1, 4), (2, 8)), jnp.float32)
    ice_area = jnp.clip(0.15 + 0.049999997 * jax.random.uniform(splits[4], (NCAT, NY, NX), jnp.float32) ** block_scale(splits[4], (NCAT, NY, NX), ((1, 4), (2, 8)), -0.2, 0.2), 0.15, 0.2)
    ice_volume = jnp.clip(0.05 + 0.55 * jax.random.uniform(splits[5], (NCAT, NY, NX), jnp.float32) ** block_scale(splits[5], (NCAT, NY, NX), ((1, 4), (2, 8)), -0.2, 0.2), 0.05, 0.6)
    inverse_width = jnp.clip(jnp.exp(math.log(1.4) - 0.6931472 * jax.random.uniform(splits[6], (NY, NX), jnp.float32) ** block_scale(splits[6], (NY, NX), ((0, 4), (1, 8)), -0.2, 0.2)), 0.7, 1.4)
    inverse_height = jnp.clip(jnp.exp(math.log(1.4) - 0.6931472 * jax.random.uniform(splits[7], (NY, NX), jnp.float32) ** block_scale(splits[7], (NY, NX), ((0, 4), (1, 8)), -0.2, 0.2)), 0.7, 1.4)
    land_block = place_ends((jax.random.randint(splits[8], (NBY, NBX), 0, 4) < 3).astype(jnp.int32), jax.random.fold_in(splits[8], 1), 0, 1)
    ice_block = place_ends((jax.random.randint(splits[9], (NBY, NBX), 0, 3) < 2).astype(jnp.int32), jax.random.fold_in(splits[9], 1), 0, 1)
    writer = place_ends(jax.random.randint(splits[10], (GROUPS,), 0, SLOTS), jax.random.fold_in(splits[10], 1), 0, SLOTS - 1).astype(jnp.int32)
    return {"velocity_start": velocity_start, "stress_start": stress_start, "wind_stress": wind_stress, "ocean_current": ocean_current, "ice_area": ice_area, "ice_volume": ice_volume, "inverse_width": inverse_width, "inverse_height": inverse_height, "land_block": land_block, "ice_block": ice_block, "writer": writer}


strength_scale = 4.0
hibler_decay = 20.0
mass_rate = 16.0
water_drag = 1.0
coriolis = 0.5
relax_rate = 0.5
ellipse_square = 4.0
delta_margin = 0.5

def expand_blocks(blocks, height, breadth):
    counted = blocks.astype(jnp.float32)
    block_rows, block_cols = counted.shape
    spread = jnp.broadcast_to(counted[:, None, :, None], (block_rows, height // block_rows, block_cols, breadth // block_cols))
    return spread.reshape(height, breadth)

def stress_update(stresses, strength, across_scale, along_scale, north_east, north_west, south_east, south_west):
    grad_ux = 0.5 * across_scale * (north_east[0] + south_east[0] - (north_west[0] + south_west[0]))
    grad_vy = 0.5 * along_scale * (north_east[1] + north_west[1] - (south_east[1] + south_west[1]))
    grad_uy = 0.5 * along_scale * (north_east[0] + north_west[0] - (south_east[0] + south_west[0]))
    grad_vx = 0.5 * across_scale * (north_east[1] + south_east[1] - (north_west[1] + south_west[1]))
    divergence = grad_ux + grad_vy
    tension = grad_ux - grad_vy
    shearing = grad_uy + grad_vx
    deform = jnp.sqrt(divergence * divergence + (tension * tension + shearing * shearing) / ellipse_square)
    viscous = strength / (deform + delta_margin)
    normal_sum = (stresses[0] + relax_rate * viscous * (divergence - deform)) / (1.0 + relax_rate)
    normal_diff = (stresses[1] + relax_rate * viscous * tension / ellipse_square) / (1.0 + relax_rate)
    shear_new = (stresses[2] + relax_rate * viscous * shearing / (2.0 * ellipse_square)) / (1.0 + relax_rate)
    return jnp.stack([normal_sum, normal_diff, shear_new])

def normal_xx(stresses):
    return 0.5 * (stresses[0] + stresses[1])

def normal_yy(stresses):
    return 0.5 * (stresses[0] - stresses[1])

def stress_force(across_scale, along_scale, south_west, south_east, north_west, north_east):
    force_x = 0.5 * across_scale * (normal_xx(south_east) + normal_xx(north_east) - (normal_xx(south_west) + normal_xx(north_west))) + 0.5 * along_scale * (north_west[2] + north_east[2] - (south_west[2] + south_east[2]))
    force_y = 0.5 * across_scale * (south_east[2] + north_east[2] - (south_west[2] + north_west[2])) + 0.5 * along_scale * (normal_yy(north_west) + normal_yy(north_east) - (normal_yy(south_west) + normal_yy(south_east)))
    return (force_x, force_y)

def momentum(velocity, force_x, force_y, inertia, turning, wind_stress, ocean_current, land_cells, ice_cells):
    damped = inertia + water_drag
    right_x = inertia * velocity[0] + force_x + wind_stress[0] + water_drag * ocean_current[0]
    right_y = inertia * velocity[1] + force_y + wind_stress[1] + water_drag * ocean_current[1]
    denominator = damped * damped + turning * turning
    next_u = (damped * right_x + turning * right_y) / denominator
    next_v = (damped * right_y - turning * right_x) / denominator
    moving = jnp.stack([next_u, next_v])
    return land_cells * (ice_cells * moving + (1.0 - ice_cells) * ocean_current)

def shift_south(stacked):
    return jnp.concatenate([jnp.zeros_like(stacked[:, :1]), stacked[:, :-1]], axis=1)

def fold_north(stacked):
    return jnp.concatenate([stacked[:, 1:], stacked[:, -1:, ::-1]], axis=1)

def reference(velocity_start, stress_start, wind_stress, ocean_current, ice_area, ice_volume, inverse_width, inverse_height, land_block, ice_block, writer):
    height, breadth = inverse_width.shape
    land_cells = expand_blocks(land_block, height, breadth)
    ice_cells = expand_blocks(ice_block, height, breadth)
    area_total = lax.optimization_barrier(jnp.sum(ice_area, axis=0))
    volume_total = lax.optimization_barrier(jnp.sum(ice_volume, axis=0))
    strength = strength_scale * volume_total * jnp.exp(-hibler_decay * (1.0 - area_total)) * land_cells
    inertia = mass_rate * (1.0 + volume_total)
    turning = coriolis * (1.0 + volume_total)
    velocity = velocity_start
    stresses = stress_start
    for subcycle in range(SUB):
        west_side = jnp.roll(velocity, 1, axis=2)
        south_side = shift_south(velocity)
        south_west = shift_south(west_side)
        stresses = stress_update(stresses, strength, inverse_width, inverse_height, velocity, west_side, south_side, south_west)
        east_side = jnp.roll(stresses, -1, axis=2)
        north_side = fold_north(stresses)
        north_east = jnp.roll(north_side, -1, axis=2)
        force_x, force_y = stress_force(inverse_width, inverse_height, stresses, east_side, north_side, north_east)
        velocity = momentum(velocity, force_x, force_y, inertia, turning, wind_stress, ocean_current, land_cells, ice_cells)
    snapshot = jnp.concatenate([ice_area, ice_volume], axis=0)
    strip_owner = writer[jnp.arange(NX, dtype=jnp.int32) // CX]
    slot_index = jnp.arange(SLOTS, dtype=jnp.int32)
    chosen = slot_index[:, None, None, None] == strip_owner[None, None, None, :]
    restart = jnp.where(chosen, snapshot[None], jnp.zeros((), snapshot.dtype))
    return (velocity, stresses, restart)
```

```python
import functools

import jax
import jax.numpy as jnp
from jax import lax
from jax.experimental import pallas as pl
from jax.experimental.pallas import tpu as pltpu
from jax.sharding import PartitionSpec as P

SUB = 12
PAD = 8
LANES = 16
FIELDS = 13

strength_scale = 4.0
hibler_decay = 20.0
mass_rate = 16.0
water_drag = 1.0
coriolis = 0.5


def halo_rows():
    return -(-SUB // 8) * 8


def expand_into(mask_ref, blocks_ref):
    block_rows, block_cols = blocks_ref.shape
    height, breadth = mask_ref.shape
    tall, wide = height // block_rows, breadth // block_cols
    counted = blocks_ref[...].astype(jnp.float32)
    lane = lax.broadcasted_iota(jnp.int32, (block_rows, breadth), 1)
    spread = jnp.zeros((block_rows, breadth), jnp.float32)
    for b in range(block_cols):
        inside = (lane >= b * wide) & (lane < (b + 1) * wide)
        spread = jnp.where(inside, counted[:, b : b + 1], spread)
    for b in range(block_rows):
        mask_ref[b * tall : (b + 1) * tall, :] = jnp.broadcast_to(
            spread[b : b + 1, :], (tall, breadth)
        )


def kernel(
    nr,
    nc,
    vel_ref,
    str_ref,
    wind_ref,
    cur_ref,
    area_ref,
    vol_ref,
    iw_ref,
    ih_ref,
    land_ref,
    ice_ref,
    vel_out,
    str_out,
    strips,
    main,
    side,
    pack_e,
    pack_w,
    land_e,
    land_w,
    ocean_ref,
    icy_ref,
    send_sem,
    recv_sem,
    x_send,
    x_recv,
    f_send,
    f_recv,
    own_sem,
):
    hr = halo_rows()
    height, breadth = iw_ref.shape
    cats = area_ref.shape[0]
    rows = height + 2 * hr
    per = breadth // LANES
    groups = pack_e.shape[0]
    r = lax.axis_index("row")
    c = lax.axis_index("col")
    east = lax.rem(c + 1, nc)
    west = lax.rem(c + nc - 1, nc)
    mirror = nc - 1 - c
    m_e = lax.rem(mirror + nc - 1, nc)
    m_w = lax.rem(mirror + 1, nc)
    partner = r + 1 - 2 * lax.rem(r, 2)
    is_top = r == nr - 1
    not_top = r < nr - 1
    above_bottom = r > 0
    self_e = jnp.logical_and(is_top, m_e == c)
    self_w = jnp.logical_and(is_top, m_w == c)
    other_e = jnp.logical_and(is_top, m_e != c)
    other_w = jnp.logical_and(is_top, m_w != c)
    others = [lax.rem(r + 2 * k, nr) for k in range(1, nr // 2)]

    barrier = pltpu.get_barrier_semaphore()

    def greet(row, col):
        pl.semaphore_signal(
            barrier,
            inc=1,
            device_id={"row": row, "col": col},
            device_id_type=pl.DeviceIdType.MESH,
        )

    greet(r, east)
    greet(r, west)
    greet(partner, c)
    for other in others:
        greet(other, c)

    @pl.when(not_top)
    def _():
        greet(r + 1, c)
        greet(r + 1, east)
        greet(r + 1, west)

    @pl.when(above_bottom)
    def _():
        greet(r - 1, c)
        greet(r - 1, east)
        greet(r - 1, west)

    @pl.when(is_top)
    def _():
        greet(r, mirror)

    @pl.when(other_e)
    def _():
        greet(r, m_e)

    @pl.when(other_w)
    def _():
        greet(r, m_w)

    own = pl.ds(pl.multiple_of(r * height, height), height)
    locals_ = [
        pltpu.make_async_copy(area_ref, strips.at[0:cats, own, :], own_sem.at[0]),
        pltpu.make_async_copy(vol_ref, strips.at[cats : 2 * cats, own, :], own_sem.at[1]),
    ]
    for copy in locals_:
        copy.start()

    expand_into(ocean_ref, land_ref)
    expand_into(icy_ref, ice_ref)
    first = PAD + hr
    lane = lax.broadcasted_iota(jnp.int32, (8, breadth), 1)
    zero = jnp.zeros((8, breadth), jnp.float32)
    for f in range(5):
        for at in (0, PAD + rows):
            main[f, at : at + 8, :] = zero
            side[f, at : at + 8, :] = zero
    for k in range(height // 8):
        here = slice(8 * k, 8 * k + 8)
        there = slice(first + 8 * k, first + 8 * k + 8)
        area = area_ref[0, here, :]
        volume = vol_ref[0, here, :]
        for n in range(1, cats):
            area = area + area_ref[n, here, :]
            volume = volume + vol_ref[n, here, :]
        ocean = ocean_ref[here, :]
        icy = icy_ref[here, :]
        strength = strength_scale * volume * jnp.exp(-hibler_decay * (1.0 - area)) * ocean
        inertia = mass_rate * (1.0 + volume)
        turning = coriolis * (1.0 + volume)
        damped = inertia + water_drag
        live = ocean * icy / (damped * damped + turning * turning)
        ca = damped * live
        cb = turning * live
        rest = ocean * (1.0 - icy)
        cu = cur_ref[0, here, :]
        cv = cur_ref[1, here, :]
        gu = wind_ref[0, here, :] + water_drag * cu
        gv = wind_ref[1, here, :] + water_drag * cv
        values = [
            vel_ref[0, here, :],
            vel_ref[1, here, :],
            str_ref[0, here, :],
            str_ref[1, here, :],
            str_ref[2, here, :],
            ca * gu + cb * gv + rest * cu,
            ca * gv - cb * gu + rest * cv,
            ca,
            cb,
            inertia,
            strength * (1.0 / 3.0),
            0.5 * iw_ref[here, :],
            0.5 * ih_ref[here, :],
        ]
        for f, value in enumerate(values):
            main[f, there, :] = value
        for g in range(groups):
            packed_e = zero
            packed_w = zero
            for s in range(per):
                f = g * per + s
                if f >= FIELDS:
                    break
                slot = (lane >= s * LANES) & (lane < (s + 1) * LANES)
                value = values[f]
                turn_w = s * LANES
                turn_e = (s * LANES + LANES) % breadth
                packed_w = jnp.where(
                    slot, pltpu.roll(value, turn_w, 1) if turn_w else value, packed_w
                )
                packed_e = jnp.where(
                    slot, pltpu.roll(value, turn_e, 1) if turn_e else value, packed_e
                )
            pack_e[g, here, :] = packed_e
            pack_w[g, here, :] = packed_w

    peers = 3 + len(others) + 3 * not_top.astype(jnp.int32) + 3 * above_bottom.astype(jnp.int32)
    peers = peers + is_top.astype(jnp.int32)
    peers = peers + other_e.astype(jnp.int32) + other_w.astype(jnp.int32)
    pl.semaphore_wait(barrier, peers)

    def remote(src, dst, send, recv, row, col):
        return pltpu.make_async_remote_copy(
            src_ref=src,
            dst_ref=dst,
            send_sem=send,
            recv_sem=recv,
            device_id={"row": row, "col": col},
            device_id_type=pl.DeviceIdType.MESH,
        )

    mid = slice(hr, hr + height)
    low = slice(0, hr)
    high = slice(hr + height, rows)
    top_rows = slice(height - hr, height)
    bottom_rows = slice(0, hr)

    def halo(slot, src, dst, row, col):
        return remote(src, dst, send_sem.at[slot], recv_sem.at[slot], row, col)

    to_west = halo(0, pack_w, land_e.at[:, mid, :], r, west)
    to_east = halo(1, pack_e, land_w.at[:, mid, :], r, east)
    main_top = main.at[:, first + height - hr : first + height, :]
    main_bottom = main.at[:, first : first + hr, :]
    main_south = main.at[:, PAD : PAD + hr, :]
    main_north = main.at[:, first + height : first + height + hr, :]
    up = [
        halo(2, main_top, main_south, r + 1, c),
        halo(4, pack_w.at[:, top_rows, :], land_e.at[:, low, :], r + 1, west),
        halo(5, pack_e.at[:, top_rows, :], land_w.at[:, low, :], r + 1, east),
    ]
    down = [
        halo(3, main_bottom, main_north, r - 1, c),
        halo(6, pack_w.at[:, bottom_rows, :], land_e.at[:, high, :], r - 1, west),
        halo(7, pack_e.at[:, bottom_rows, :], land_w.at[:, high, :], r - 1, east),
    ]
    over = remote(main_top, main_north, send_sem.at[8], recv_sem.at[3], r, mirror)
    over_w = remote(
        pack_w.at[:, top_rows, :], land_e.at[:, high, :], send_sem.at[9], recv_sem.at[6], r, m_w
    )
    over_e = remote(
        pack_e.at[:, top_rows, :], land_w.at[:, high, :], send_sem.at[10], recv_sem.at[7], r, m_e
    )

    @pl.when(is_top)
    def _():
        over.start()

    @pl.when(other_w)
    def _():
        over_w.start()

    @pl.when(other_e)
    def _():
        over_e.start()

    @pl.when(self_w)
    def _():
        land_e[:, high, :] = pack_w[:, top_rows, :]

    @pl.when(self_e)
    def _():
        land_w[:, high, :] = pack_e[:, top_rows, :]

    to_west.start()
    to_east.start()

    @pl.when(not_top)
    def _():
        for copy in up:
            copy.start()

    @pl.when(above_bottom)
    def _():
        for copy in down:
            copy.start()

    crossing = []
    for k, other in enumerate(others):
        for part, ref in enumerate((area_ref, vol_ref)):
            crossing.append(
                remote(
                    ref,
                    strips.at[part * cats : (part + 1) * cats, own, :],
                    x_send.at[2 * k + part],
                    x_recv.at[2 * k + part],
                    other,
                    c,
                )
            )
    for copy in crossing:
        copy.start()
    forwards = []
    for part, ref in enumerate((area_ref, vol_ref)):
        forwards.append(
            remote(
                ref,
                strips.at[part * cats : (part + 1) * cats, own, :],
                f_send.at[part],
                f_recv.at[part],
                partner,
                c,
            )
        )
    for copy in forwards:
        copy.start()

    @pl.when(r == 0)
    def _():
        for f in range(FIELDS):
            main[f, PAD : PAD + hr, :] = jnp.zeros((hr, breadth), jnp.float32)
        for g in range(groups):
            land_e[g, low, :] = jnp.zeros((hr, breadth), jnp.float32)
            land_w[g, low, :] = jnp.zeros((hr, breadth), jnp.float32)

    to_west.wait()
    to_east.wait()

    @pl.when(not_top)
    def _():
        for copy in up:
            copy.wait_send()
        for copy in down:
            copy.wait_recv()

    @pl.when(above_bottom)
    def _():
        for copy in down:
            copy.wait_send()
        for copy in up:
            copy.wait_recv()

    @pl.when(is_top)
    def _():
        over.wait()

    @pl.when(other_w)
    def _():
        over_w.wait()

    @pl.when(other_e)
    def _():
        over_e.wait()

    for k in range(rows // 8):
        here = slice(8 * k, 8 * k + 8)
        there = slice(PAD + 8 * k, PAD + 8 * k + 8)
        for f in range(FIELDS):
            g, s = divmod(f, per)
            turn_e = (breadth - s * LANES) % breadth
            turn_w = (breadth - LANES - s * LANES) % breadth
            from_e = land_e[g, here, :]
            from_w = land_w[g, here, :]
            from_e = pltpu.roll(from_e, turn_e, 1) if turn_e else from_e
            from_w = pltpu.roll(from_w, turn_w, 1) if turn_w else from_w
            side[f, there, :] = jnp.where(
                lane < LANES, from_e, jnp.where(lane >= breadth - LANES, from_w, 0.0)
            )

    sub = lax.broadcasted_iota(jnp.int32, (8, breadth), 0)
    first_lane = lane == 0
    last_lane = lane == breadth - 1
    fold_here = (sub == 7) & is_top
    backwards = breadth - 1 - lane

    def west_of(a, b):
        ra = pltpu.roll(a, 1, 1)
        rb = pltpu.roll(b, 1, 1)
        return jnp.where(first_lane, rb, ra), jnp.where(first_lane, ra, rb)

    def east_of(a, b):
        ra = pltpu.roll(a, breadth - 1, 1)
        rb = pltpu.roll(b, breadth - 1, 1)
        return jnp.where(last_lane, rb, ra), jnp.where(last_lane, ra, rb)

    tiles = (main, side)
    last_own = first + height - 1
    last_north = PAD + rows - 1

    def cycle(_, carry):
        for k in range(rows // 8):
            here = slice(PAD + 8 * k, PAD + 8 * k + 8)
            south = slice(PAD + 8 * k - 1, PAD + 8 * k + 7)
            us, ud, vs, vd = [], [], [], []
            for t in tiles:
                u, v = t[0, here, :], t[1, here, :]
                su, sv = t[0, south, :], t[1, south, :]
                us.append(u + su)
                ud.append(u - su)
                vs.append(v + sv)
                vd.append(v - sv)
            wus, wud, wvs, wvd = west_of(*us), west_of(*ud), west_of(*vs), west_of(*vd)
            for i, t in enumerate(tiles):
                hw, hh = t[11, here, :], t[12, here, :]
                gux = hw * (us[i] - wus[i])
                gvx = hw * (vs[i] - wvs[i])
                guy = hh * (ud[i] + wud[i])
                gvy = hh * (vd[i] + wvd[i])
                div = gux + gvy
                ten = gux - gvy
                shear = guy + gvx
                deform = jnp.sqrt(div * div + 0.25 * (ten * ten + shear * shear))
                w = t[10, here, :] / (deform + 0.5)
                t[2, here, :] = t[2, here, :] * (2.0 / 3.0) + w * (div - deform)
                t[3, here, :] = t[3, here, :] * (2.0 / 3.0) + (0.25 * w) * ten
                t[4, here, :] = t[4, here, :] * (2.0 / 3.0) + (0.125 * w) * shear

        def edge(row):
            lines = [t[f, row : row + 1, :] for t in tiles for f in (2, 3, 4)]
            stacked = jnp.concatenate(lines + [lines[0], lines[0]], axis=0)
            return jnp.take_along_axis(stacked, backwards, axis=1)

        own_edge = edge(last_own)
        north_edge = edge(last_north)
        for i, t in enumerate(tiles):
            for f in range(3):
                line = 3 * i + f
                t[2 + f, last_north + 1 : last_north + 2, :] = own_edge[line : line + 1, :]

        for k in range(rows // 8):
            here = slice(PAD + 8 * k, PAD + 8 * k + 8)
            north = slice(PAD + 8 * k + 1, PAD + 8 * k + 9)
            p, d, q, e = [], [], [], []
            for i, t in enumerate(tiles):
                s1, s2, s12 = t[2, here, :], t[3, here, :], t[4, here, :]
                n1, n2, n12 = t[2, north, :], t[3, north, :], t[4, north, :]
                if PAD + 8 * k + 7 == last_own:
                    ghost = [
                        jnp.broadcast_to(
                            north_edge[3 * i + f : 3 * i + f + 1, :], (8, breadth)
                        )
                        for f in range(3)
                    ]
                    n1 = jnp.where(fold_here, ghost[0], n1)
                    n2 = jnp.where(fold_here, ghost[1], n2)
                    n12 = jnp.where(fold_here, ghost[2], n12)
                p.append((s1 + s2) + (n1 + n2))
                d.append(n12 - s12)
                q.append(s12 + n12)
                e.append((n1 - n2) - (s1 - s2))
            ep, ed, eq, ee = east_of(*p), east_of(*d), east_of(*q), east_of(*e)
            for i, t in enumerate(tiles):
                hw, hh = t[11, here, :], t[12, here, :]
                fx = hw * (0.5 * (ep[i] - p[i])) + hh * (d[i] + ed[i])
                fy = hw * (eq[i] - q[i]) + hh * (0.5 * (e[i] + ee[i]))
                inertia = t[9, here, :]
                rx = inertia * t[0, here, :] + fx
                ry = inertia * t[1, here, :] + fy
                ca, cb = t[7, here, :], t[8, here, :]
                t[0, here, :] = ca * rx + cb * ry + t[5, here, :]
                t[1, here, :] = ca * ry - cb * rx + t[6, here, :]
        return carry

    early = SUB * 3 // 4
    lax.fori_loop(0, early, cycle, 0)

    relays = []
    for k in range(len(others)):
        source = lax.rem(r + nr - 2 * (k + 1), nr)
        lines = pl.ds(pl.multiple_of(source * height, height), height)
        for part in range(2):
            crossing[2 * k + part].wait_recv()
            block = strips.at[part * cats : (part + 1) * cats, lines, :]
            slot = 2 + 2 * k + part
            copy = remote(block, block, f_send.at[slot], f_recv.at[slot], partner, c)
            copy.start()
            relays.append(copy)

    lax.fori_loop(0, SUB - early, cycle, 0)

    inner = slice(first, first + height)
    for f in range(2):
        vel_out[f] = main[f, inner, :]
    for f in range(3):
        str_out[f] = main[2 + f, inner, :]

    for copy in locals_:
        copy.wait()
    for copy in crossing:
        copy.wait_send()
    for copy in forwards + relays:
        copy.wait()


def shards(nr, nc, *operands):
    (vel, stress, wind, current, area, volume, iw, ih, land, ice, writer) = operands
    hr = halo_rows()
    height, breadth = iw.shape
    cats = area.shape[0]
    rows = height + 2 * hr
    groups = -(-FIELDS // (breadth // LANES))
    space = pl.BlockSpec(memory_space=pltpu.VMEM)
    relayed = max(2 * (nr // 2 - 1), 1)
    f32 = jnp.float32
    sent = 4 * (2 * FIELDS * hr * breadth + 2 * groups * rows * breadth + 3 * area.size)
    velocity, stresses, strips = pl.pallas_call(
        functools.partial(kernel, nr, nc),
        out_shape=(
            jax.ShapeDtypeStruct(vel.shape, f32),
            jax.ShapeDtypeStruct(stress.shape, f32),
            jax.ShapeDtypeStruct((2 * cats, nr * height, breadth), f32),
        ),
        in_specs=[space] * 10,
        out_specs=(space, space, space),
        scratch_shapes=[
            pltpu.VMEM((FIELDS, rows + 2 * PAD, breadth), f32),
            pltpu.VMEM((FIELDS, rows + 2 * PAD, breadth), f32),
            pltpu.VMEM((groups, height, breadth), f32),
            pltpu.VMEM((groups, height, breadth), f32),
            pltpu.VMEM((groups, rows, breadth), f32),
            pltpu.VMEM((groups, rows, breadth), f32),
            pltpu.VMEM((height, breadth), f32),
            pltpu.VMEM((height, breadth), f32),
            pltpu.SemaphoreType.DMA((11,)),
            pltpu.SemaphoreType.DMA((8,)),
            pltpu.SemaphoreType.DMA((relayed,)),
            pltpu.SemaphoreType.DMA((relayed,)),
            pltpu.SemaphoreType.DMA((2 + relayed,)),
            pltpu.SemaphoreType.DMA((2 + relayed,)),
            pltpu.SemaphoreType.DMA((2,)),
        ],
        compiler_params=pltpu.CompilerParams(
            collective_id=0, has_side_effects=True, vmem_limit_bytes=32 * 1024 * 1024
        ),
        cost_estimate=pl.CostEstimate(
            flops=SUB * rows * breadth * 200, bytes_accessed=sent, transcendentals=0
        ),
    )(vel, stress, wind, current, area, volume, iw, ih, land, ice)
    index = jnp.arange(writer.shape[0], dtype=jnp.int32)
    chosen = jnp.sum(jnp.where(index == lax.axis_index("col"), writer, 0))
    restart = jnp.where(chosen == lax.axis_index("row"), strips, 0.0)[None]
    return velocity, stresses, restart


def solution(mesh):
    field = P(None, "row", "col")
    flat = P("row", "col")
    return jax.shard_map(
        functools.partial(shards, mesh.shape["row"], mesh.shape["col"]),
        mesh=mesh,
        in_specs=(field,) * 6 + (flat,) * 4 + (P(),),
        out_specs=(field, field, P("row", None, None, "col")),
        check_vma=False,
    )
```

```python
import functools

import jax
import jax.numpy as jnp
from jax import lax
from jax.experimental import pallas as pl
from jax.experimental.pallas import tpu as pltpu
from jax.sharding import PartitionSpec as P

SUB = 12
PAD = 8
LANES = 16
FIELDS = 13

strength_scale = 4.0
hibler_decay = 20.0
mass_rate = 16.0
water_drag = 1.0
coriolis = 0.5


def halo_rows():
    return -(-SUB // 8) * 8


def expand_into(mask_ref, blocks_ref):
    block_cols, block_rows = blocks_ref.shape
    height, breadth = mask_ref.shape
    tall, wide = height // block_rows, breadth // block_cols
    counted = blocks_ref[...].astype(jnp.float32)
    start = wide * lax.broadcasted_iota(jnp.int32, (block_cols, breadth), 0)
    lane = lax.broadcasted_iota(jnp.int32, (block_cols, breadth), 1)
    inside = (lane >= start) & (lane < start + wide)
    for b in range(block_rows):
        spread = jnp.where(inside, counted[:, b : b + 1], 0.0)
        line = jnp.sum(spread, axis=0, keepdims=True)
        mask_ref[b * tall : (b + 1) * tall, :] = jnp.broadcast_to(line, (tall, breadth))


def kernel(
    nr,
    nc,
    vel_in,
    str_in,
    wind_in,
    cur_in,
    area_in,
    vol_in,
    iw_in,
    ih_in,
    land_in,
    ice_in,
    writer_in,
    vel_out,
    str_out,
    strips,
    writer_out,
    vel_ref,
    str_ref,
    wind_ref,
    cur_ref,
    iw_ref,
    ih_ref,
    land_ref,
    ice_ref,
    main,
    side,
    pack_e,
    pack_w,
    land_e,
    land_w,
    ocean_ref,
    icy_ref,
    send_sem,
    recv_sem,
    x_send,
    x_recv,
    f_send,
    f_recv,
    in_sem,
):
    hr = halo_rows()
    height, breadth = iw_ref.shape
    cats = area_in.shape[0]
    rows = height + 2 * hr
    per = breadth // LANES
    groups = pack_e.shape[0]
    r = lax.axis_index("row")
    c = lax.axis_index("col")
    east = lax.rem(c + 1, nc)
    west = lax.rem(c + nc - 1, nc)
    mirror = nc - 1 - c
    m_e = lax.rem(mirror + nc - 1, nc)
    m_w = lax.rem(mirror + 1, nc)
    partner = r + 1 - 2 * lax.rem(r, 2)
    is_top = r == nr - 1
    not_top = r < nr - 1
    above_bottom = r > 0
    self_e = jnp.logical_and(is_top, m_e == c)
    self_w = jnp.logical_and(is_top, m_w == c)
    other_e = jnp.logical_and(is_top, m_e != c)
    other_w = jnp.logical_and(is_top, m_w != c)
    others = [lax.rem(r + 2 * k, nr) for k in range(1, nr // 2)]

    own = pl.ds(pl.multiple_of(r * height, height), height)
    area_own = strips.at[0:cats, own, :]
    vol_own = strips.at[cats : 2 * cats, own, :]
    inputs = (
        (area_in, area_own),
        (vol_in, vol_own),
        (land_in, land_ref),
        (ice_in, ice_ref),
        (vel_in, vel_ref),
        (str_in, str_ref),
        (wind_in, wind_ref),
        (cur_in, cur_ref),
        (iw_in, iw_ref),
        (ih_in, ih_ref),
        (writer_in, writer_out),
    )
    arriving = [
        pltpu.make_async_copy(src, dst, in_sem.at[n]) for n, (src, dst) in enumerate(inputs)
    ]
    for copy in arriving:
        copy.start()

    barrier = pltpu.get_barrier_semaphore()

    def greet(row, col):
        pl.semaphore_signal(
            barrier,
            inc=1,
            device_id={"row": row, "col": col},
            device_id_type=pl.DeviceIdType.MESH,
        )

    greet(r, east)
    greet(r, west)
    greet(partner, c)
    for other in others:
        greet(other, c)

    @pl.when(not_top)
    def _():
        greet(r + 1, c)
        greet(r + 1, east)
        greet(r + 1, west)

    @pl.when(above_bottom)
    def _():
        greet(r - 1, c)
        greet(r - 1, east)
        greet(r - 1, west)

    @pl.when(is_top)
    def _():
        greet(r, mirror)

    @pl.when(other_e)
    def _():
        greet(r, m_e)

    @pl.when(other_w)
    def _():
        greet(r, m_w)

    first = PAD + hr
    lane = lax.broadcasted_iota(jnp.int32, (8, breadth), 1)
    zero = jnp.zeros((8, breadth), jnp.float32)
    for f in range(5):
        for at in (0, PAD + rows):
            main[f, at : at + 8, :] = zero
            side[f, at : at + 8, :] = zero
    for copy in arriving:
        copy.wait()
    expand_into(ocean_ref, land_ref)
    expand_into(icy_ref, ice_ref)
    for k in range(height // 8):
        here = slice(8 * k, 8 * k + 8)
        there = slice(first + 8 * k, first + 8 * k + 8)
        lines = pl.ds(pl.multiple_of(r * height + 8 * k, 8), 8)
        area = strips[0, lines, :]
        volume = strips[cats, lines, :]
        for n in range(1, cats):
            area = area + strips[n, lines, :]
            volume = volume + strips[cats + n, lines, :]
        ocean = ocean_ref[here, :]
        icy = icy_ref[here, :]
        strength = strength_scale * volume * jnp.exp(-hibler_decay * (1.0 - area)) * ocean
        inertia = mass_rate * (1.0 + volume)
        turning = coriolis * (1.0 + volume)
        damped = inertia + water_drag
        live = ocean * icy / (damped * damped + turning * turning)
        ca = damped * live
        cb = turning * live
        rest = ocean * (1.0 - icy)
        cu = cur_ref[0, here, :]
        cv = cur_ref[1, here, :]
        gu = wind_ref[0, here, :] + water_drag * cu
        gv = wind_ref[1, here, :] + water_drag * cv
        values = [
            vel_ref[0, here, :],
            vel_ref[1, here, :],
            str_ref[0, here, :],
            str_ref[1, here, :],
            str_ref[2, here, :],
            ca * gu + cb * gv + rest * cu,
            ca * gv - cb * gu + rest * cv,
            ca,
            cb,
            inertia,
            strength * (1.0 / 3.0),
            0.5 * iw_ref[here, :],
            0.5 * ih_ref[here, :],
        ]
        for f, value in enumerate(values):
            main[f, there, :] = value
        for g in range(groups):
            packed_e = zero
            packed_w = zero
            for s in range(per):
                f = g * per + s
                if f >= FIELDS:
                    break
                slot = (lane >= s * LANES) & (lane < (s + 1) * LANES)
                value = values[f]
                turn_w = s * LANES
                turn_e = (s * LANES + LANES) % breadth
                packed_w = jnp.where(
                    slot, pltpu.roll(value, turn_w, 1) if turn_w else value, packed_w
                )
                packed_e = jnp.where(
                    slot, pltpu.roll(value, turn_e, 1) if turn_e else value, packed_e
                )
            pack_e[g, here, :] = packed_e
            pack_w[g, here, :] = packed_w

    peers = 3 + len(others) + 3 * not_top.astype(jnp.int32) + 3 * above_bottom.astype(jnp.int32)
    peers = peers + is_top.astype(jnp.int32)
    peers = peers + other_e.astype(jnp.int32) + other_w.astype(jnp.int32)
    pl.semaphore_wait(barrier, peers)

    def remote(src, dst, send, recv, row, col):
        return pltpu.make_async_remote_copy(
            src_ref=src,
            dst_ref=dst,
            send_sem=send,
            recv_sem=recv,
            device_id={"row": row, "col": col},
            device_id_type=pl.DeviceIdType.MESH,
        )

    mid = slice(hr, hr + height)
    low = slice(0, hr)
    high = slice(hr + height, rows)
    top_rows = slice(height - hr, height)
    bottom_rows = slice(0, hr)

    def halo(slot, src, dst, row, col):
        return remote(src, dst, send_sem.at[slot], recv_sem.at[slot], row, col)

    to_west = halo(0, pack_w, land_e.at[:, mid, :], r, west)
    to_east = halo(1, pack_e, land_w.at[:, mid, :], r, east)
    main_top = main.at[:, first + height - hr : first + height, :]
    main_bottom = main.at[:, first : first + hr, :]
    main_south = main.at[:, PAD : PAD + hr, :]
    main_north = main.at[:, first + height : first + height + hr, :]
    up = [
        halo(2, main_top, main_south, r + 1, c),
        halo(4, pack_w.at[:, top_rows, :], land_e.at[:, low, :], r + 1, west),
        halo(5, pack_e.at[:, top_rows, :], land_w.at[:, low, :], r + 1, east),
    ]
    down = [
        halo(3, main_bottom, main_north, r - 1, c),
        halo(6, pack_w.at[:, bottom_rows, :], land_e.at[:, high, :], r - 1, west),
        halo(7, pack_e.at[:, bottom_rows, :], land_w.at[:, high, :], r - 1, east),
    ]
    over = remote(main_top, main_north, send_sem.at[8], recv_sem.at[3], r, mirror)
    over_w = remote(
        pack_w.at[:, top_rows, :], land_e.at[:, high, :], send_sem.at[9], recv_sem.at[6], r, m_w
    )
    over_e = remote(
        pack_e.at[:, top_rows, :], land_w.at[:, high, :], send_sem.at[10], recv_sem.at[7], r, m_e
    )

    @pl.when(is_top)
    def _():
        over.start()

    @pl.when(other_w)
    def _():
        over_w.start()

    @pl.when(other_e)
    def _():
        over_e.start()

    @pl.when(self_w)
    def _():
        land_e[:, high, :] = pack_w[:, top_rows, :]

    @pl.when(self_e)
    def _():
        land_w[:, high, :] = pack_e[:, top_rows, :]

    to_west.start()
    to_east.start()

    @pl.when(not_top)
    def _():
        for copy in up:
            copy.start()

    @pl.when(above_bottom)
    def _():
        for copy in down:
            copy.start()

    crossing = []
    for k, other in enumerate(others):
        for part, ref in enumerate((area_own, vol_own)):
            crossing.append(
                remote(
                    ref,
                    ref,
                    x_send.at[2 * k + part],
                    x_recv.at[2 * k + part],
                    other,
                    c,
                )
            )
    for copy in crossing:
        copy.start()
    forwards = []
    for part, ref in enumerate((area_own, vol_own)):
        forwards.append(
            remote(
                ref,
                ref,
                f_send.at[part],
                f_recv.at[part],
                partner,
                c,
            )
        )
    for copy in forwards:
        copy.start()

    @pl.when(r == 0)
    def _():
        for f in range(FIELDS):
            main[f, PAD : PAD + hr, :] = jnp.zeros((hr, breadth), jnp.float32)
        for g in range(groups):
            land_e[g, low, :] = jnp.zeros((hr, breadth), jnp.float32)
            land_w[g, low, :] = jnp.zeros((hr, breadth), jnp.float32)

    to_west.wait()
    to_east.wait()

    @pl.when(not_top)
    def _():
        for copy in up:
            copy.wait_send()
        for copy in down:
            copy.wait_recv()

    @pl.when(above_bottom)
    def _():
        for copy in down:
            copy.wait_send()
        for copy in up:
            copy.wait_recv()

    @pl.when(is_top)
    def _():
        over.wait()

    @pl.when(other_w)
    def _():
        over_w.wait()

    @pl.when(other_e)
    def _():
        over_e.wait()

    for k in range(rows // 8):
        here = slice(8 * k, 8 * k + 8)
        there = slice(PAD + 8 * k, PAD + 8 * k + 8)
        for f in range(FIELDS):
            g, s = divmod(f, per)
            turn_e = (breadth - s * LANES) % breadth
            turn_w = (breadth - LANES - s * LANES) % breadth
            from_e = land_e[g, here, :]
            from_w = land_w[g, here, :]
            from_e = pltpu.roll(from_e, turn_e, 1) if turn_e else from_e
            from_w = pltpu.roll(from_w, turn_w, 1) if turn_w else from_w
            side[f, there, :] = jnp.where(
                lane < LANES, from_e, jnp.where(lane >= breadth - LANES, from_w, 0.0)
            )

    sub = lax.broadcasted_iota(jnp.int32, (8, breadth), 0)
    first_lane = lane == 0
    last_lane = lane == breadth - 1
    fold_here = (sub == 7) & is_top
    backwards = breadth - 1 - lane

    def west_of(a, b):
        ra = pltpu.roll(a, 1, 1)
        rb = pltpu.roll(b, 1, 1)
        return jnp.where(first_lane, rb, ra), jnp.where(first_lane, ra, rb)

    def east_of(a, b):
        ra = pltpu.roll(a, breadth - 1, 1)
        rb = pltpu.roll(b, breadth - 1, 1)
        return jnp.where(last_lane, rb, ra), jnp.where(last_lane, ra, rb)

    tiles = (main, side)
    last_own = first + height - 1
    last_north = PAD + rows - 1

    def cycle(_, carry):
        for k in range(rows // 8):
            here = slice(PAD + 8 * k, PAD + 8 * k + 8)
            south = slice(PAD + 8 * k - 1, PAD + 8 * k + 7)
            us, ud, vs, vd = [], [], [], []
            for t in tiles:
                u, v = t[0, here, :], t[1, here, :]
                su, sv = t[0, south, :], t[1, south, :]
                us.append(u + su)
                ud.append(u - su)
                vs.append(v + sv)
                vd.append(v - sv)
            wus, wud, wvs, wvd = west_of(*us), west_of(*ud), west_of(*vs), west_of(*vd)
            for i, t in enumerate(tiles):
                hw, hh = t[11, here, :], t[12, here, :]
                gux = hw * (us[i] - wus[i])
                gvx = hw * (vs[i] - wvs[i])
                guy = hh * (ud[i] + wud[i])
                gvy = hh * (vd[i] + wvd[i])
                div = gux + gvy
                ten = gux - gvy
                shear = guy + gvx
                deform = jnp.sqrt(div * div + 0.25 * (ten * ten + shear * shear))
                w = t[10, here, :] / (deform + 0.5)
                t[2, here, :] = t[2, here, :] * (2.0 / 3.0) + w * (div - deform)
                t[3, here, :] = t[3, here, :] * (2.0 / 3.0) + (0.25 * w) * ten
                t[4, here, :] = t[4, here, :] * (2.0 / 3.0) + (0.125 * w) * shear

        def edge(row):
            lines = [t[f, row : row + 1, :] for t in tiles for f in (2, 3, 4)]
            stacked = jnp.concatenate(lines + [lines[0], lines[0]], axis=0)
            return jnp.take_along_axis(stacked, backwards, axis=1)

        own_edge = edge(last_own)
        north_edge = edge(last_north)
        for i, t in enumerate(tiles):
            for f in range(3):
                line = 3 * i + f
                t[2 + f, last_north + 1 : last_north + 2, :] = own_edge[line : line + 1, :]

        for k in range(rows // 8):
            here = slice(PAD + 8 * k, PAD + 8 * k + 8)
            north = slice(PAD + 8 * k + 1, PAD + 8 * k + 9)
            p, d, q, e = [], [], [], []
            for i, t in enumerate(tiles):
                s1, s2, s12 = t[2, here, :], t[3, here, :], t[4, here, :]
                n1, n2, n12 = t[2, north, :], t[3, north, :], t[4, north, :]
                if PAD + 8 * k + 7 == last_own:
                    ghost = [
                        jnp.broadcast_to(
                            north_edge[3 * i + f : 3 * i + f + 1, :], (8, breadth)
                        )
                        for f in range(3)
                    ]
                    n1 = jnp.where(fold_here, ghost[0], n1)
                    n2 = jnp.where(fold_here, ghost[1], n2)
                    n12 = jnp.where(fold_here, ghost[2], n12)
                p.append((s1 + s2) + (n1 + n2))
                d.append(n12 - s12)
                q.append(s12 + n12)
                e.append((n1 - n2) - (s1 - s2))
            ep, ed, eq, ee = east_of(*p), east_of(*d), east_of(*q), east_of(*e)
            for i, t in enumerate(tiles):
                hw, hh = t[11, here, :], t[12, here, :]
                fx = hw * (0.5 * (ep[i] - p[i])) + hh * (d[i] + ed[i])
                fy = hw * (eq[i] - q[i]) + hh * (0.5 * (e[i] + ee[i]))
                inertia = t[9, here, :]
                rx = inertia * t[0, here, :] + fx
                ry = inertia * t[1, here, :] + fy
                ca, cb = t[7, here, :], t[8, here, :]
                t[0, here, :] = ca * rx + cb * ry + t[5, here, :]
                t[1, here, :] = ca * ry - cb * rx + t[6, here, :]
        return carry

    early = SUB * 3 // 4
    lax.fori_loop(0, early, cycle, 0)

    relays = []
    for k in range(len(others)):
        source = lax.rem(r + nr - 2 * (k + 1), nr)
        lines = pl.ds(pl.multiple_of(source * height, height), height)
        for part in range(2):
            crossing[2 * k + part].wait_recv()
            block = strips.at[part * cats : (part + 1) * cats, lines, :]
            slot = 2 + 2 * k + part
            copy = remote(block, block, f_send.at[slot], f_recv.at[slot], partner, c)
            copy.start()
            relays.append(copy)

    lax.fori_loop(0, SUB - early, cycle, 0)

    inner = slice(first, first + height)
    for f in range(2):
        vel_out[f] = main[f, inner, :]
    for f in range(3):
        str_out[f] = main[2 + f, inner, :]

    for copy in crossing:
        copy.wait_send()
    for copy in forwards + relays:
        copy.wait()


def place(strips, vel, stress, writer, restart_out, vel_out, str_out, blank, sem):
    r = lax.axis_index("row")
    c = lax.axis_index("col")
    small = [
        pltpu.make_async_copy(vel, vel_out, sem.at[0]),
        pltpu.make_async_copy(stress, str_out, sem.at[1]),
    ]
    for copy in small:
        copy.start()
    index = lax.broadcasted_iota(jnp.int32, writer.shape, 1)
    chosen = jnp.sum(jnp.where(index == c, writer[...], 0))
    fields = strips.shape[0]

    @pl.when(chosen == r)
    def _():
        copies = [
            pltpu.make_async_copy(strips.at[n], restart_out.at[0, n], sem.at[2 + n])
            for n in range(fields)
        ]
        for copy in copies:
            copy.start()
        for copy in copies:
            copy.wait()

    @pl.when(chosen != r)
    def _():
        blank[...] = jnp.zeros(blank.shape, blank.dtype)
        copies = [
            pltpu.make_async_copy(blank, restart_out.at[0, n], sem.at[2 + n])
            for n in range(fields)
        ]
        for copy in copies:
            copy.start()
        for copy in copies:
            copy.wait()

    for copy in small:
        copy.wait()


def shards(nr, nc, *operands):
    (vel, stress, wind, current, area, volume, iw, ih, land, ice, writer) = operands
    hr = halo_rows()
    height, breadth = iw.shape
    cats = area.shape[0]
    rows = height + 2 * hr
    groups = -(-FIELDS // (breadth // LANES))
    vmem = pl.BlockSpec(memory_space=pltpu.VMEM)
    hbm = pl.BlockSpec(memory_space=pltpu.HBM)
    relayed = max(2 * (nr // 2 - 1), 1)
    f32 = jnp.float32
    land, ice = land.T, ice.T
    writer = writer[None]
    inputs = [
        pltpu.with_memory_space_constraint(x, pltpu.HBM)
        for x in (vel, stress, wind, current, area, volume, iw, ih, land, ice, writer)
    ]
    sent = 4 * (2 * FIELDS * hr * breadth + 2 * groups * rows * breadth + 3 * area.size)
    velocity, stresses, strips, writer = pl.pallas_call(
        functools.partial(kernel, nr, nc),
        out_shape=(
            jax.ShapeDtypeStruct(vel.shape, f32),
            jax.ShapeDtypeStruct(stress.shape, f32),
            jax.ShapeDtypeStruct((2 * cats, nr * height, breadth), f32),
            jax.ShapeDtypeStruct(writer.shape, writer.dtype),
        ),
        in_specs=[hbm] * 11,
        out_specs=(vmem,) * 4,
        scratch_shapes=[
            pltpu.VMEM(vel.shape, f32),
            pltpu.VMEM(stress.shape, f32),
            pltpu.VMEM(wind.shape, f32),
            pltpu.VMEM(current.shape, f32),
            pltpu.VMEM(iw.shape, f32),
            pltpu.VMEM(ih.shape, f32),
            pltpu.VMEM(land.shape, land.dtype),
            pltpu.VMEM(ice.shape, ice.dtype),
            pltpu.VMEM((FIELDS, rows + 2 * PAD, breadth), f32),
            pltpu.VMEM((FIELDS, rows + 2 * PAD, breadth), f32),
            pltpu.VMEM((groups, height, breadth), f32),
            pltpu.VMEM((groups, height, breadth), f32),
            pltpu.VMEM((groups, rows, breadth), f32),
            pltpu.VMEM((groups, rows, breadth), f32),
            pltpu.VMEM((height, breadth), f32),
            pltpu.VMEM((height, breadth), f32),
            pltpu.SemaphoreType.DMA((11,)),
            pltpu.SemaphoreType.DMA((8,)),
            pltpu.SemaphoreType.DMA((relayed,)),
            pltpu.SemaphoreType.DMA((relayed,)),
            pltpu.SemaphoreType.DMA((2 + relayed,)),
            pltpu.SemaphoreType.DMA((2 + relayed,)),
            pltpu.SemaphoreType.DMA((11,)),
        ],
        compiler_params=pltpu.CompilerParams(
            collective_id=0, has_side_effects=True, vmem_limit_bytes=32 * 1024 * 1024
        ),
        cost_estimate=pl.CostEstimate(
            flops=SUB * rows * breadth * 200, bytes_accessed=sent, transcendentals=0
        ),
    )(*inputs)
    restart, velocity, stresses = pl.pallas_call(
        place,
        out_shape=(
            jax.ShapeDtypeStruct((1,) + strips.shape, f32),
            jax.ShapeDtypeStruct(vel.shape, f32),
            jax.ShapeDtypeStruct(stress.shape, f32),
        ),
        in_specs=[vmem] * 4,
        out_specs=(hbm,) * 3,
        scratch_shapes=[
            pltpu.VMEM(strips.shape[1:], f32),
            pltpu.SemaphoreType.DMA((2 + 2 * cats,)),
        ],
        compiler_params=pltpu.CompilerParams(vmem_limit_bytes=4 * 1024 * 1024),
    )(strips, velocity, stresses, writer)
    return velocity, stresses, restart


def solution(mesh):
    field = P(None, "row", "col")
    flat = P("row", "col")
    return jax.shard_map(
        functools.partial(shards, mesh.shape["row"], mesh.shape["col"]),
        mesh=mesh,
        in_specs=(field,) * 6 + (flat,) * 4 + (P(),),
        out_specs=(field, field, P("row", None, None, "col")),
        check_vma=False,
    )
```

```python
import functools

import jax
import jax.numpy as jnp
from jax import lax
from jax.experimental import pallas as pl
from jax.experimental.pallas import tpu as pltpu
from jax.sharding import PartitionSpec as P

SUB = 12
PAD = 8
LANES = 16
FIELDS = 13

strength_scale = 4.0
hibler_decay = 20.0
mass_rate = 16.0
water_drag = 1.0
coriolis = 0.5


def halo_rows():
    return -(-SUB // 8) * 8


def expand_into(mask_ref, blocks_ref):
    block_cols, block_rows = blocks_ref.shape
    height, breadth = mask_ref.shape
    tall, wide = height // block_rows, breadth // block_cols
    counted = blocks_ref[...].astype(jnp.float32)
    start = wide * lax.broadcasted_iota(jnp.int32, (block_cols, breadth), 0)
    lane = lax.broadcasted_iota(jnp.int32, (block_cols, breadth), 1)
    inside = (lane >= start) & (lane < start + wide)
    for b in range(block_rows):
        spread = jnp.where(inside, counted[:, b : b + 1], 0.0)
        line = jnp.sum(spread, axis=0, keepdims=True)
        mask_ref[b * tall : (b + 1) * tall, :] = jnp.broadcast_to(line, (tall, breadth))


def kernel(
    nr,
    nc,
    vel_in,
    str_in,
    wind_in,
    cur_in,
    area_in,
    vol_in,
    iw_in,
    ih_in,
    land_in,
    ice_in,
    writer_in,
    vel_out,
    str_out,
    strips,
    writer_out,
    vel_ref,
    str_ref,
    wind_ref,
    cur_ref,
    iw_ref,
    ih_ref,
    land_ref,
    ice_ref,
    main,
    side,
    pack_e,
    pack_w,
    land_e,
    land_w,
    ocean_ref,
    icy_ref,
    send_sem,
    recv_sem,
    x_send,
    x_recv,
    f_send,
    f_recv,
    in_sem,
):
    hr = halo_rows()
    height, breadth = iw_ref.shape
    cats = area_in.shape[0]
    rows = height + 2 * hr
    per = breadth // LANES
    groups = pack_e.shape[0]
    r = lax.axis_index("row")
    c = lax.axis_index("col")
    east = lax.rem(c + 1, nc)
    west = lax.rem(c + nc - 1, nc)
    mirror = nc - 1 - c
    m_e = lax.rem(mirror + nc - 1, nc)
    m_w = lax.rem(mirror + 1, nc)
    partner = r + 1 - 2 * lax.rem(r, 2)
    is_top = r == nr - 1
    not_top = r < nr - 1
    above_bottom = r > 0
    self_e = jnp.logical_and(is_top, m_e == c)
    self_w = jnp.logical_and(is_top, m_w == c)
    other_e = jnp.logical_and(is_top, m_e != c)
    other_w = jnp.logical_and(is_top, m_w != c)
    others = [lax.rem(r + 2 * k, nr) for k in range(1, nr // 2)]

    own = pl.ds(pl.multiple_of(r * height, height), height)
    area_own = strips.at[0:cats, own, :]
    vol_own = strips.at[cats : 2 * cats, own, :]
    inputs = (
        (area_in, area_own),
        (vol_in, vol_own),
        (land_in, land_ref),
        (ice_in, ice_ref),
        (vel_in, vel_ref),
        (str_in, str_ref),
        (wind_in, wind_ref),
        (cur_in, cur_ref),
        (iw_in, iw_ref),
        (ih_in, ih_ref),
        (writer_in, writer_out),
    )
    arriving = [
        pltpu.make_async_copy(src, dst, in_sem.at[n]) for n, (src, dst) in enumerate(inputs)
    ]
    for copy in arriving:
        copy.start()

    barrier = pltpu.get_barrier_semaphore()

    def greet(row, col):
        pl.semaphore_signal(
            barrier,
            inc=1,
            device_id={"row": row, "col": col},
            device_id_type=pl.DeviceIdType.MESH,
        )

    greet(r, east)
    greet(r, west)
    greet(partner, c)
    for other in others:
        greet(other, c)

    @pl.when(not_top)
    def _():
        greet(r + 1, c)
        greet(r + 1, east)
        greet(r + 1, west)

    @pl.when(above_bottom)
    def _():
        greet(r - 1, c)
        greet(r - 1, east)
        greet(r - 1, west)

    @pl.when(is_top)
    def _():
        greet(r, mirror)

    @pl.when(other_e)
    def _():
        greet(r, m_e)

    @pl.when(other_w)
    def _():
        greet(r, m_w)

    first = PAD + hr
    lane = lax.broadcasted_iota(jnp.int32, (8, breadth), 1)
    zero = jnp.zeros((8, breadth), jnp.float32)
    for f in range(5):
        for at in (0, PAD + rows):
            main[f, at : at + 8, :] = zero
            side[f, at : at + 8, :] = zero
    arriving[0].wait()
    arriving[1].wait()

    peers = 3 + len(others) + 3 * not_top.astype(jnp.int32) + 3 * above_bottom.astype(jnp.int32)
    peers = peers + is_top.astype(jnp.int32)
    peers = peers + other_e.astype(jnp.int32) + other_w.astype(jnp.int32)
    pl.semaphore_wait(barrier, peers)

    def remote(src, dst, send, recv, row, col):
        return pltpu.make_async_remote_copy(
            src_ref=src,
            dst_ref=dst,
            send_sem=send,
            recv_sem=recv,
            device_id={"row": row, "col": col},
            device_id_type=pl.DeviceIdType.MESH,
        )

    crossing = [
        remote(
            strips.at[n, own, :],
            strips.at[n, own, :],
            x_send.at[n * len(others) + k],
            x_recv.at[n * len(others) + k],
            other,
            c,
        )
        for n in range(2 * cats)
        for k, other in enumerate(others)
    ]
    for copy in crossing[: len(others)]:
        copy.start()
    for copy in arriving[2:]:
        copy.wait()
    expand_into(ocean_ref, land_ref)
    expand_into(icy_ref, ice_ref)
    for k in range(height // 8):
        here = slice(8 * k, 8 * k + 8)
        there = slice(first + 8 * k, first + 8 * k + 8)
        lines = pl.ds(pl.multiple_of(r * height + 8 * k, 8), 8)
        area = strips[0, lines, :]
        volume = strips[cats, lines, :]
        for n in range(1, cats):
            area = area + strips[n, lines, :]
            volume = volume + strips[cats + n, lines, :]
        ocean = ocean_ref[here, :]
        icy = icy_ref[here, :]
        strength = strength_scale * volume * jnp.exp(-hibler_decay * (1.0 - area)) * ocean
        inertia = mass_rate * (1.0 + volume)
        turning = coriolis * (1.0 + volume)
        damped = inertia + water_drag
        live = ocean * icy / (damped * damped + turning * turning)
        ca = damped * live
        cb = turning * live
        rest = ocean * (1.0 - icy)
        cu = cur_ref[0, here, :]
        cv = cur_ref[1, here, :]
        gu = wind_ref[0, here, :] + water_drag * cu
        gv = wind_ref[1, here, :] + water_drag * cv
        values = [
            vel_ref[0, here, :],
            vel_ref[1, here, :],
            str_ref[0, here, :],
            str_ref[1, here, :],
            str_ref[2, here, :],
            ca * gu + cb * gv + rest * cu,
            ca * gv - cb * gu + rest * cv,
            ca,
            cb,
            inertia,
            strength * (1.0 / 3.0),
            0.5 * iw_ref[here, :],
            0.5 * ih_ref[here, :],
        ]
        for f, value in enumerate(values):
            main[f, there, :] = value
        for g in range(groups):
            packed_e = zero
            packed_w = zero
            for s in range(per):
                f = g * per + s
                if f >= FIELDS:
                    break
                slot = (lane >= s * LANES) & (lane < (s + 1) * LANES)
                value = values[f]
                turn_w = s * LANES
                turn_e = (s * LANES + LANES) % breadth
                packed_w = jnp.where(
                    slot, pltpu.roll(value, turn_w, 1) if turn_w else value, packed_w
                )
                packed_e = jnp.where(
                    slot, pltpu.roll(value, turn_e, 1) if turn_e else value, packed_e
                )
            pack_e[g, here, :] = packed_e
            pack_w[g, here, :] = packed_w

    mid = slice(hr, hr + height)
    low = slice(0, hr)
    high = slice(hr + height, rows)
    top_rows = slice(height - hr, height)
    bottom_rows = slice(0, hr)

    def halo(slot, src, dst, row, col):
        return remote(src, dst, send_sem.at[slot], recv_sem.at[slot], row, col)

    to_west = halo(0, pack_w, land_e.at[:, mid, :], r, west)
    to_east = halo(1, pack_e, land_w.at[:, mid, :], r, east)
    main_top = main.at[:, first + height - hr : first + height, :]
    main_bottom = main.at[:, first : first + hr, :]
    main_south = main.at[:, PAD : PAD + hr, :]
    main_north = main.at[:, first + height : first + height + hr, :]
    up = [
        halo(2, main_top, main_south, r + 1, c),
        halo(4, pack_w.at[:, top_rows, :], land_e.at[:, low, :], r + 1, west),
        halo(5, pack_e.at[:, top_rows, :], land_w.at[:, low, :], r + 1, east),
    ]
    down = [
        halo(3, main_bottom, main_north, r - 1, c),
        halo(6, pack_w.at[:, bottom_rows, :], land_e.at[:, high, :], r - 1, west),
        halo(7, pack_e.at[:, bottom_rows, :], land_w.at[:, high, :], r - 1, east),
    ]
    over = remote(main_top, main_north, send_sem.at[8], recv_sem.at[3], r, mirror)
    over_w = remote(
        pack_w.at[:, top_rows, :], land_e.at[:, high, :], send_sem.at[9], recv_sem.at[6], r, m_w
    )
    over_e = remote(
        pack_e.at[:, top_rows, :], land_w.at[:, high, :], send_sem.at[10], recv_sem.at[7], r, m_e
    )

    @pl.when(is_top)
    def _():
        over.start()

    @pl.when(other_w)
    def _():
        over_w.start()

    @pl.when(other_e)
    def _():
        over_e.start()

    @pl.when(self_w)
    def _():
        land_e[:, high, :] = pack_w[:, top_rows, :]

    @pl.when(self_e)
    def _():
        land_w[:, high, :] = pack_e[:, top_rows, :]

    to_west.start()
    to_east.start()

    @pl.when(not_top)
    def _():
        for copy in up:
            copy.start()

    @pl.when(above_bottom)
    def _():
        for copy in down:
            copy.start()

    for copy in crossing[len(others) :]:
        copy.start()
    forward = remote(
        strips.at[:, own, :], strips.at[:, own, :], f_send.at[0], f_recv.at[0], partner, c
    )
    forward.start()

    @pl.when(r == 0)
    def _():
        for f in range(FIELDS):
            main[f, PAD : PAD + hr, :] = jnp.zeros((hr, breadth), jnp.float32)
        for g in range(groups):
            land_e[g, low, :] = jnp.zeros((hr, breadth), jnp.float32)
            land_w[g, low, :] = jnp.zeros((hr, breadth), jnp.float32)

    to_west.wait()
    to_east.wait()

    @pl.when(not_top)
    def _():
        for copy in up:
            copy.wait_send()
        for copy in down:
            copy.wait_recv()

    @pl.when(above_bottom)
    def _():
        for copy in down:
            copy.wait_send()
        for copy in up:
            copy.wait_recv()

    @pl.when(is_top)
    def _():
        over.wait()

    @pl.when(other_w)
    def _():
        over_w.wait()

    @pl.when(other_e)
    def _():
        over_e.wait()

    for k in range(rows // 8):
        here = slice(8 * k, 8 * k + 8)
        there = slice(PAD + 8 * k, PAD + 8 * k + 8)
        for f in range(FIELDS):
            g, s = divmod(f, per)
            turn_e = (breadth - s * LANES) % breadth
            turn_w = (breadth - LANES - s * LANES) % breadth
            from_e = land_e[g, here, :]
            from_w = land_w[g, here, :]
            from_e = pltpu.roll(from_e, turn_e, 1) if turn_e else from_e
            from_w = pltpu.roll(from_w, turn_w, 1) if turn_w else from_w
            side[f, there, :] = jnp.where(
                lane < LANES, from_e, jnp.where(lane >= breadth - LANES, from_w, 0.0)
            )

    sub = lax.broadcasted_iota(jnp.int32, (8, breadth), 0)
    first_lane = lane == 0
    last_lane = lane == breadth - 1
    fold_here = (sub == 7) & is_top
    backwards = breadth - 1 - lane

    def west_of(a, b):
        ra = pltpu.roll(a, 1, 1)
        rb = pltpu.roll(b, 1, 1)
        return jnp.where(first_lane, rb, ra), jnp.where(first_lane, ra, rb)

    def east_of(a, b):
        ra = pltpu.roll(a, breadth - 1, 1)
        rb = pltpu.roll(b, breadth - 1, 1)
        return jnp.where(last_lane, rb, ra), jnp.where(last_lane, ra, rb)

    tiles = (main, side)
    last_own = first + height - 1
    last_north = PAD + rows - 1

    def cycle(low_chunk):
        for k in range(low_chunk, rows // 8):
            here = slice(PAD + 8 * k, PAD + 8 * k + 8)
            south = slice(PAD + 8 * k - 1, PAD + 8 * k + 7)
            us, ud, vs, vd = [], [], [], []
            for t in tiles:
                u, v = t[0, here, :], t[1, here, :]
                su, sv = t[0, south, :], t[1, south, :]
                us.append(u + su)
                ud.append(u - su)
                vs.append(v + sv)
                vd.append(v - sv)
            wus, wud, wvs, wvd = west_of(*us), west_of(*ud), west_of(*vs), west_of(*vd)
            for i, t in enumerate(tiles):
                hw, hh = t[11, here, :], t[12, here, :]
                gux = hw * (us[i] - wus[i])
                gvx = hw * (vs[i] - wvs[i])
                guy = hh * (ud[i] + wud[i])
                gvy = hh * (vd[i] + wvd[i])
                div = gux + gvy
                ten = gux - gvy
                shear = guy + gvx
                deform = jnp.sqrt(div * div + 0.25 * (ten * ten + shear * shear))
                w = t[10, here, :] / (deform + 0.5)
                t[2, here, :] = t[2, here, :] * (2.0 / 3.0) + w * (div - deform)
                t[3, here, :] = t[3, here, :] * (2.0 / 3.0) + (0.25 * w) * ten
                t[4, here, :] = t[4, here, :] * (2.0 / 3.0) + (0.125 * w) * shear

        def edge(row):
            lines = [t[f, row : row + 1, :] for t in tiles for f in (2, 3, 4)]
            stacked = jnp.concatenate(lines + [lines[0], lines[0]], axis=0)
            return jnp.take_along_axis(stacked, backwards, axis=1)

        own_edge = edge(last_own)
        north_edge = edge(last_north)
        for i, t in enumerate(tiles):
            for f in range(3):
                line = 3 * i + f
                t[2 + f, last_north + 1 : last_north + 2, :] = own_edge[line : line + 1, :]

        for k in range(low_chunk, rows // 8):
            here = slice(PAD + 8 * k, PAD + 8 * k + 8)
            north = slice(PAD + 8 * k + 1, PAD + 8 * k + 9)
            p, d, q, e = [], [], [], []
            for i, t in enumerate(tiles):
                s1, s2, s12 = t[2, here, :], t[3, here, :], t[4, here, :]
                n1, n2, n12 = t[2, north, :], t[3, north, :], t[4, north, :]
                if PAD + 8 * k + 7 == last_own:
                    ghost = [
                        jnp.broadcast_to(
                            north_edge[3 * i + f : 3 * i + f + 1, :], (8, breadth)
                        )
                        for f in range(3)
                    ]
                    n1 = jnp.where(fold_here, ghost[0], n1)
                    n2 = jnp.where(fold_here, ghost[1], n2)
                    n12 = jnp.where(fold_here, ghost[2], n12)
                p.append((s1 + s2) + (n1 + n2))
                d.append(n12 - s12)
                q.append(s12 + n12)
                e.append((n1 - n2) - (s1 - s2))
            ep, ed, eq, ee = east_of(*p), east_of(*d), east_of(*q), east_of(*e)
            for i, t in enumerate(tiles):
                hw, hh = t[11, here, :], t[12, here, :]
                fx = hw * (0.5 * (ep[i] - p[i])) + hh * (d[i] + ed[i])
                fy = hw * (eq[i] - q[i]) + hh * (0.5 * (e[i] + ee[i]))
                inertia = t[9, here, :]
                rx = inertia * t[0, here, :] + fx
                ry = inertia * t[1, here, :] + fy
                ca, cb = t[7, here, :], t[8, here, :]
                t[0, here, :] = ca * rx + cb * ry + t[5, here, :]
                t[1, here, :] = ca * ry - cb * rx + t[6, here, :]

    def relays(n):
        copies = []
        for k in range(len(others)):
            source = lax.rem(r + nr - 2 * (k + 1), nr)
            lines = pl.ds(pl.multiple_of(source * height, height), height)
            block = strips.at[n, lines, :]
            slot = n * len(others) + k
            copies.append(
                remote(block, block, f_send.at[1 + slot], f_recv.at[1 + slot], partner, c)
            )
        return copies

    def relay(fields):
        for n in fields:
            for k, copy in enumerate(relays(n)):
                crossing[n * len(others) + k].wait_recv()
                copy.start()

    early = SUB - 8 - 1
    count = 2 * cats

    def early_cycle(i, carry):
        cycle(0)
        return carry

    def late_cycle(i, carry):
        @pl.when(i == SUB // 2)
        def _():
            relay(range(0, count // 2))

        @pl.when(i == SUB * 3 // 4)
        def _():
            relay(range(count // 2, count * 4 // 5))

        cycle((hr - 8) // 8)
        return carry

    lax.fori_loop(0, early, early_cycle, 0)
    lax.fori_loop(early, SUB, late_cycle, 0)
    relay(range(count * 4 // 5, count))

    inner = slice(first, first + height)
    for f in range(2):
        vel_out[f] = main[f, inner, :]
    for f in range(3):
        str_out[f] = main[2 + f, inner, :]

    for copy in crossing:
        copy.wait_send()
    forward.wait()
    for n in range(count):
        for copy in relays(n):
            copy.wait()


def place(strips, vel, stress, writer, restart_out, vel_out, str_out, blank, sem):
    r = lax.axis_index("row")
    c = lax.axis_index("col")
    small = [
        pltpu.make_async_copy(vel, vel_out, sem.at[0]),
        pltpu.make_async_copy(stress, str_out, sem.at[1]),
    ]
    for copy in small:
        copy.start()
    index = lax.broadcasted_iota(jnp.int32, writer.shape, 1)
    chosen = jnp.sum(jnp.where(index == c, writer[...], 0))
    fields = strips.shape[0]

    @pl.when(chosen == r)
    def _():
        copies = [
            pltpu.make_async_copy(strips.at[n], restart_out.at[0, n], sem.at[2 + n])
            for n in range(fields)
        ]
        for copy in copies:
            copy.start()
        for copy in copies:
            copy.wait()

    @pl.when(chosen != r)
    def _():
        blank[...] = jnp.zeros(blank.shape, blank.dtype)
        copies = [
            pltpu.make_async_copy(blank, restart_out.at[0, n], sem.at[2 + n])
            for n in range(fields)
        ]
        for copy in copies:
            copy.start()
        for copy in copies:
            copy.wait()

    for copy in small:
        copy.wait()


def shards(nr, nc, *operands):
    (vel, stress, wind, current, area, volume, iw, ih, land, ice, writer) = operands
    hr = halo_rows()
    height, breadth = iw.shape
    cats = area.shape[0]
    rows = height + 2 * hr
    groups = -(-FIELDS // (breadth // LANES))
    vmem = pl.BlockSpec(memory_space=pltpu.VMEM)
    hbm = pl.BlockSpec(memory_space=pltpu.HBM)
    relayed = max(2 * cats * (nr // 2 - 1), 1)
    f32 = jnp.float32
    land, ice = land.T, ice.T
    writer = writer[None]
    inputs = [
        pltpu.with_memory_space_constraint(x, pltpu.HBM)
        for x in (vel, stress, wind, current, area, volume, iw, ih, land, ice, writer)
    ]
    sent = 4 * (2 * FIELDS * hr * breadth + 2 * groups * rows * breadth + 3 * area.size)
    velocity, stresses, strips, writer = pl.pallas_call(
        functools.partial(kernel, nr, nc),
        out_shape=(
            jax.ShapeDtypeStruct(vel.shape, f32),
            jax.ShapeDtypeStruct(stress.shape, f32),
            jax.ShapeDtypeStruct((2 * cats, nr * height, breadth), f32),
            jax.ShapeDtypeStruct(writer.shape, writer.dtype),
        ),
        in_specs=[hbm] * 11,
        out_specs=(vmem,) * 4,
        scratch_shapes=[
            pltpu.VMEM(vel.shape, f32),
            pltpu.VMEM(stress.shape, f32),
            pltpu.VMEM(wind.shape, f32),
            pltpu.VMEM(current.shape, f32),
            pltpu.VMEM(iw.shape, f32),
            pltpu.VMEM(ih.shape, f32),
            pltpu.VMEM(land.shape, land.dtype),
            pltpu.VMEM(ice.shape, ice.dtype),
            pltpu.VMEM((FIELDS, rows + 2 * PAD, breadth), f32),
            pltpu.VMEM((FIELDS, rows + 2 * PAD, breadth), f32),
            pltpu.VMEM((groups, height, breadth), f32),
            pltpu.VMEM((groups, height, breadth), f32),
            pltpu.VMEM((groups, rows, breadth), f32),
            pltpu.VMEM((groups, rows, breadth), f32),
            pltpu.VMEM((height, breadth), f32),
            pltpu.VMEM((height, breadth), f32),
            pltpu.SemaphoreType.DMA((11,)),
            pltpu.SemaphoreType.DMA((8,)),
            pltpu.SemaphoreType.DMA((relayed,)),
            pltpu.SemaphoreType.DMA((relayed,)),
            pltpu.SemaphoreType.DMA((1 + relayed,)),
            pltpu.SemaphoreType.DMA((1 + relayed,)),
            pltpu.SemaphoreType.DMA((11,)),
        ],
        compiler_params=pltpu.CompilerParams(
            collective_id=0, has_side_effects=True, vmem_limit_bytes=32 * 1024 * 1024
        ),
        cost_estimate=pl.CostEstimate(
            flops=SUB * rows * breadth * 200, bytes_accessed=sent, transcendentals=0
        ),
    )(*inputs)
    restart, velocity, stresses = pl.pallas_call(
        place,
        out_shape=(
            jax.ShapeDtypeStruct((1,) + strips.shape, f32),
            jax.ShapeDtypeStruct(vel.shape, f32),
            jax.ShapeDtypeStruct(stress.shape, f32),
        ),
        in_specs=[vmem] * 4,
        out_specs=(hbm,) * 3,
        scratch_shapes=[
            pltpu.VMEM(strips.shape[1:], f32),
            pltpu.SemaphoreType.DMA((2 + 2 * cats,)),
        ],
        compiler_params=pltpu.CompilerParams(vmem_limit_bytes=4 * 1024 * 1024),
    )(strips, velocity, stresses, writer)
    return velocity, stresses, restart


def solution(mesh):
    field = P(None, "row", "col")
    flat = P("row", "col")
    return jax.shard_map(
        functools.partial(shards, mesh.shape["row"], mesh.shape["col"]),
        mesh=mesh,
        in_specs=(field,) * 6 + (flat,) * 4 + (P(),),
        out_specs=(field, field, P("row", None, None, "col")),
        check_vma=False,
    )
```
